32 devices in a mesh: tensor: 2 (over x), context: 8 (over z, core), dp: 2 (over y).
Axes of the slice: x: 2, y: 2, z: 4, core: 2. Of those that a mesh axis runs over, the one named last changes fastest.
Arguments:
- query_a: bfloat16 [2048, 1024], P(('dp', 'context'), 'tensor'), parts along dimension 0, may hold values from -5 to 5
- key_a: bfloat16 [2048, 256], P(('dp', 'context'), 'tensor'), parts along dimension 0, may hold values from -5 to 5
- value_a: bfloat16 [2048, 256], P(('dp', 'context'), 'tensor'), parts along dimension 0, may hold values from -12 to 12
- grad_out_a: bfloat16 [2048, 1024], P(('dp', 'context'), 'tensor'), parts along dimension 0, may hold values from -6 to 6
- query_b: bfloat16 [2048, 1024], P(('dp', 'context'), 'tensor'), parts along dimension 0, may hold values from -5 to 5
- key_b: bfloat16 [2048, 256], P(('dp', 'context'), 'tensor'), parts along dimension 0, may hold values from -5 to 5
- value_b: bfloat16 [2048, 256], P(('dp', 'context'), 'tensor'), parts along dimension 0, may hold values from -12 to 12
- slab_owner: int32 [8], replicated, may hold values from 0 to 7, each once
Outputs:
- out_b: bfloat16 [2048, 1024], P(('dp', 'context'), 'tensor'), parts along dimension 0
- grad_query_a: bfloat16 [2048, 1024], P(('dp', 'context'), 'tensor'), parts along dimension 0
- grad_key_a: bfloat16 [2048, 256], P(('dp', 'context'), 'tensor'), parts along dimension 0
- grad_value_a: bfloat16 [2048, 256], P(('dp', 'context'), 'tensor'), parts along dimension 0
The draws below stay inside these ranges and needn't reach their ends.
There are 2 independent parts, one for each index of `dp`. The reference program is written for one: setup_inputs(seed, part) draws one part's arguments, and reference() takes and returns one part's arrays. A program takes and returns all parts, laid end to end along the dimension named above; an argument that names none is the same for every part. Nothing has to cross between parts.
Inputs may be any that keep to these rules, and one draw needn't show every extreme that they name: `slab_owner`: each number appears once.
All inputs are finite; a program needn't handle non-finite values.
Results may differ from the reference program's by a relative error of at most 0.0091.
Values may be sent and summed in bfloat16 or wider, within the bound.
A program may use at most 64 MiB of HBM per device.

```python
import jax
import jax.numpy as jnp
from jax import lax

HEAD_DIM = 128
HEADS_DEV = 4
TOK_DEV = 128
HEADS = 8
KV_HEADS = 2
TOKENS = 1024
N_CONTEXT = 8


def random_base(key, label, width):
    inner = jax.random.fold_in(key, label)
    return jnp.clip(1.4 * jax.random.normal(inner, (TOKENS, width), jnp.float32), -5.0, 5.0)


def drawn_queries(key, label):
    values = random_base(key, label + 1, HEADS * HEAD_DIM)
    return values.astype(jnp.bfloat16)


def drawn_keys(key, label):
    values = random_base(key, label + 7, KV_HEADS * HEAD_DIM)
    return values.astype(jnp.bfloat16)


def draw_query_a(key, part):
    return drawn_queries(key, 101)


def draw_key_a(key, part):
    return drawn_keys(key, 101)


def draw_query_b(key, part):
    return drawn_queries(key, 202)


def draw_key_b(key, part):
    return drawn_keys(key, 202)


def steps_of(stream_key, dims, cuts, low, top_value):
    level, own = 1.0, jax.random.fold_in(stream_key, 6)
    for position, shards_of in cuts:
        steps = jnp.exp(jax.random.uniform(jax.random.fold_in(own, position), (shards_of,), jnp.float32, low / len(cuts), top_value / len(cuts)))
        level = level * jnp.repeat(steps, dims[position] // shards_of).reshape([-1 if axis == position else 1 for axis in range(len(dims))])
    return level


def bell_draw(own_key, shape, spread, reach, pieces=(), held_as=jnp.bfloat16):
    drawn = jax.random.normal(own_key, shape, jnp.float32) * spread
    if len(pieces) > 0:
        drawn = steps_of(own_key, shape, pieces, -0.22, 0.18) * drawn
    return jnp.clip(drawn, min=-reach, max=reach).astype(held_as)


def setup_inputs(seed: int = 0, part: int = 0) -> dict:
    key_of = jax.random.split(jax.random.key(seed), 9)
    own_keys = jax.random.split(jax.random.fold_in(key_of[8], part), 9)
    query_a = draw_query_a(jax.random.fold_in(jax.random.fold_in(key_of[8], part), 71), part)
    key_a = draw_key_a(jax.random.fold_in(jax.random.fold_in(key_of[8], part), 71), part)
    value_a = bell_draw(own_keys[2], (TOKENS, KV_HEADS * HEAD_DIM), 2.0, 12.0, ((0, 8), (1, 2)))
    grad_out_a = bell_draw(own_keys[3], (TOKENS, HEADS * HEAD_DIM), 1.0, 6.0, ((0, 8), (1, 2)))
    query_b = draw_query_b(jax.random.fold_in(jax.random.fold_in(key_of[8], part), 71), part)
    key_b = draw_key_b(jax.random.fold_in(jax.random.fold_in(key_of[8], part), 71), part)
    value_b = bell_draw(own_keys[6], (TOKENS, KV_HEADS * HEAD_DIM), 2.0, 12.0, ((0, 8), (1, 2)))
    slab_owner = jax.random.permutation(key_of[7], N_CONTEXT).astype(jnp.int32)
    return {"query_a": query_a, "key_a": key_a, "value_a": value_a, "grad_out_a": grad_out_a, "query_b": query_b, "key_b": key_b, "value_b": value_b, "slab_owner": slab_owner}


def slab_places(slab_owner):
    half = TOK_DEV // 2
    rows = jnp.arange(TOKENS, dtype=jnp.int32)
    holder = rows // TOK_DEV
    within = rows % TOK_DEV
    owner_slab = slab_owner[holder].astype(jnp.int32)
    slab = jnp.where(within < half, owner_slab, 2 * N_CONTEXT - 1 - owner_slab)
    return (slab * half + within % half).astype(jnp.int32)


def scores_of(queries, keys, query_places, places):
    raw = jnp.einsum("bhd,nd->hbn", queries.astype(jnp.float32), keys.astype(jnp.float32))
    allowed = places[None, None, :] <= query_places[None, :, None]
    return raw * HEAD_DIM ** -0.5, allowed


def forward_rows(queries, query_places, keys, values, places):
    scaled, allowed = scores_of(queries, keys, query_places, places)
    top = jnp.max(jnp.where(allowed, scaled, -jnp.inf), axis=2)
    raised = jnp.where(allowed, jnp.exp(scaled - top[:, :, None]), 0.0)
    total = jnp.sum(raised, axis=2)
    weights = lax.optimization_barrier(raised.astype(jnp.bfloat16))
    summed = jnp.einsum("hbn,nd->bhd", weights.astype(jnp.float32), values.astype(jnp.float32))
    mixed = summed / jnp.transpose(total)[:, :, None]
    return mixed, jnp.transpose(top + jnp.log(total))


def forward_all(queries, keys, values, places):
    query_rows = min(512, TOKENS)
    blocks = TOKENS // query_rows

    def one_block(item):
        return forward_rows(item[0], item[1], keys, values, places)

    mixed, log_total = lax.map(one_block, (queries.reshape(blocks, query_rows, HEADS_DEV, HEAD_DIM), places.reshape(blocks, query_rows)))
    return mixed.reshape(TOKENS, HEADS_DEV, HEAD_DIM), log_total.reshape(TOKENS, HEADS_DEV)


def backward_all(queries, keys, values, grads, places):
    mixed, log_total = forward_all(queries, keys, values, places)
    delta = jnp.sum(grads.astype(jnp.float32) * mixed, axis=2)
    query_rows = min(512, TOKENS)
    blocks = TOKENS // query_rows
    scale = HEAD_DIM ** -0.5

    def advance(carried, item):
        block_query, block_grad, block_places, block_log, block_delta = item
        scaled, allowed = scores_of(block_query, keys, block_places, places)
        prob = jnp.where(allowed, jnp.exp(scaled - jnp.transpose(block_log)[:, :, None]), 0.0)
        prob_grad = jnp.einsum("bhd,nd->hbn", block_grad.astype(jnp.float32), values.astype(jnp.float32))
        score_grad = (prob * (prob_grad - jnp.transpose(block_delta)[:, :, None])).astype(jnp.bfloat16)
        low_prob = prob.astype(jnp.bfloat16)
        score_grad, low_prob = lax.optimization_barrier((score_grad, low_prob))
        query_grad = jnp.einsum("hbn,nd->bhd", score_grad.astype(jnp.float32), keys.astype(jnp.float32)) * scale
        key_sum = carried[0] + jnp.einsum("hbn,bhd->nd", score_grad.astype(jnp.float32), block_query.astype(jnp.float32))
        value_sum = carried[1] + jnp.einsum("hbn,bhd->nd", low_prob.astype(jnp.float32), block_grad.astype(jnp.float32))
        return (key_sum, value_sum), query_grad.astype(jnp.bfloat16)

    items = (queries.reshape(blocks, query_rows, HEADS_DEV, HEAD_DIM), grads.reshape(blocks, query_rows, HEADS_DEV, HEAD_DIM), places.reshape(blocks, query_rows), log_total.reshape(blocks, query_rows, HEADS_DEV), delta.reshape(blocks, query_rows, HEADS_DEV))
    empty = jnp.zeros((TOKENS, HEAD_DIM), jnp.float32)
    sums, query_grad = lax.scan(advance, (empty, empty), items)
    key_grad = (sums[0] * scale).astype(jnp.bfloat16)
    value_grad = sums[1].astype(jnp.bfloat16)
    return query_grad.reshape(TOKENS, HEADS_DEV * HEAD_DIM), key_grad, value_grad


def reference(query_a, key_a, value_a, grad_out_a, query_b, key_b, value_b, slab_owner):
    places = slab_places(slab_owner)
    width = HEADS_DEV * HEAD_DIM
    outs_b = []
    grads_query = []
    grads_key = []
    grads_value = []
    for group in range(KV_HEADS):
        head_lo = group * width
        kv_lo = group * HEAD_DIM
        group_query_b = query_b[:, head_lo:head_lo + width].reshape(TOKENS, HEADS_DEV, HEAD_DIM)
        mixed_b, unused = forward_all(group_query_b, key_b[:, kv_lo:kv_lo + HEAD_DIM], value_b[:, kv_lo:kv_lo + HEAD_DIM], places)
        outs_b.append(mixed_b.reshape(TOKENS, width).astype(jnp.bfloat16))
        group_query_a = query_a[:, head_lo:head_lo + width].reshape(TOKENS, HEADS_DEV, HEAD_DIM)
        group_grad = grad_out_a[:, head_lo:head_lo + width].reshape(TOKENS, HEADS_DEV, HEAD_DIM)
        query_grad, key_grad, value_grad = backward_all(group_query_a, key_a[:, kv_lo:kv_lo + HEAD_DIM], value_a[:, kv_lo:kv_lo + HEAD_DIM], group_grad, places)
        grads_query.append(query_grad)
        grads_key.append(key_grad)
        grads_value.append(value_grad)
    return (jnp.concatenate(outs_b, axis=1), jnp.concatenate(grads_query, axis=1), jnp.concatenate(grads_key, axis=1), jnp.concatenate(grads_value, axis=1))
```

```python
import functools

import jax
import jax.numpy as jnp
from jax import lax
from jax.experimental import pallas as pl
from jax.experimental.pallas import tpu as pltpu
from jax.sharding import PartitionSpec as P

LOW = -1e30
LOG2E = 1.4426950408889634
F32 = jnp.float32
BF16 = jnp.bfloat16


def dot_nt(a, b):
    return lax.dot_general(a, b, (((1,), (1,)), ((), ())), preferred_element_type=F32)


def dot_nn(a, b):
    return lax.dot_general(a, b, (((1,), (0,)), ((), ())), preferred_element_type=F32)


def dot_tn(a, b):
    return lax.dot_general(a, b, (((0,), (0,)), ((), ())), preferred_element_type=F32)


def each(lo, hi, body):
    if hi - lo <= 4:
        for t in range(lo, hi):
            body(t)
    else:
        lax.fori_loop(lo, hi, lambda t, _: (body(t), 0)[1], 0)


def kernel(
    n, tok, heads, dim,
    owner_in, qa, ka, va, ga, qb, kb, vb,
    out_b, out_dq, out_dk, out_dv,
    owner, kv, qa0, ga0, qb0, qa1, ga1, qb1,
    e_a, e_b, pg, m_a, t_a, d_a, m_b, t_b,
    st_out, st_in, glob, sb_out, sb_in,
    sg_hi, sg_lo, p_hi, p_lo, dq_own, dq_out, dq_in, ob_own, ob_out, ob_in,
    gf, gs, rp, ms, rf,
    load_sem, kv_recv, g_send, f_send, mate_send, mate_recv,
    p_send, p_recv, x_send, x_recv,
):
    chips = n // 2
    pairs = chips // 2
    half = tok // 2
    rows = heads * half
    me = lax.axis_index("context")
    chip, core = me // 2, me % 2
    mate = chip * 2 + (1 - core)
    pair, side = chip // 2, chip % 2
    partner = pair * 2 + (1 - side)
    factor = dim ** (-0.5) * LOG2E
    scale = dim ** (-0.5)
    extra = 4 * chips

    def remote(src, dst, send, recv, idx):
        return pltpu.make_async_remote_copy(
            src_ref=src, dst_ref=dst, send_sem=send, recv_sem=recv,
            device_id={"context": idx}, device_id_type=pl.DeviceIdType.MESH,
        )

    def chip_at(t):
        other = lax.rem(pair + t // 2, pairs)
        right = (other > pair).astype(jnp.int32)
        far = t % 2
        away = other * 2 + jnp.where(far == 1, right, 1 - right)
        return jnp.where(t == 0, chip, jnp.where(t == 1, partner, away))

    def is_near(d):
        return jnp.where(d > chip, side == 1, side == 0)

    def outside(d):
        return d // 2 != pair

    def kv_load(b, j):
        src = ((ka, va), (kb, vb))[b][j]
        return pltpu.make_async_copy(src, kv.at[b, j, chip], load_sem.at[b * 2 + j])

    own_rows = (qa0, ga0, qb0)
    mate_rows = (qa1, ga1, qb1)

    def row_load(i, part, h):
        src = (qa, ga, qb)[i]
        return pltpu.make_async_copy(
            src.at[pl.ds(part * half, half), pl.ds(h * dim, dim)],
            own_rows[i].at[part, pl.ds(h * half, half), :],
            load_sem.at[5 + (i * 2 + part) * heads + h],
        )

    owner_load = pltpu.make_async_copy(owner_in, owner, load_sem.at[4])

    for j in range(2):
        kv_load(0, j).start()
    owner_load.start()
    for part in range(2):
        for h in range(heads):
            row_load(0, part, h).start()
    for j in range(2):
        kv_load(1, j).start()
    for i in (1, 2):
        for part in range(2):
            for h in range(heads):
                row_load(i, part, h).start()

    barrier = pltpu.get_barrier_semaphore()
    pl.semaphore_signal(
        barrier, inc=1, device_id={"context": mate}, device_id_type=pl.DeviceIdType.MESH
    )
    count = jnp.int32(1)
    for off in range(1, chips):
        d = lax.rem(chip + off, chips)
        low, high = jnp.minimum(chip, d), jnp.maximum(chip, d)
        meet = jnp.logical_or(
            jnp.logical_not(outside(d)), jnp.logical_or(low % 2 == 1, high % 2 == 0)
        )
        count = count + meet.astype(jnp.int32)

        @pl.when(meet)
        def _():
            pl.semaphore_signal(
                barrier, inc=1, device_id={"context": d * 2 + core},
                device_id_type=pl.DeviceIdType.MESH,
            )

    def give(b, j, target):
        return remote(
            kv.at[b, j, chip], kv.at[b, j, chip], g_send.at[b, j, target],
            kv_recv.at[b, j, chip], target * 2 + core,
        )

    def nearest(k):
        other = lax.rem(pair + k, pairs)
        return other * 2 + (other < pair).astype(jnp.int32)

    def give_all(b, j):
        each(1, pairs, lambda k: give(b, j, nearest(k)).start())
        give(b, j, partner).start()

    def forward(b, j, d):
        return remote(
            kv.at[b, j, d], kv.at[b, j, d], f_send.at[b, j, d],
            kv_recv.at[b, j, d], partner * 2 + core,
        )

    def take(b, j, d):
        forward(b, j, d).wait_recv()

    def pass_on(b, j, d):
        @pl.when(jnp.logical_and(outside(d), is_near(d)))
        def _():
            forward(b, j, d).start()

    def to_mate(k):
        src, dst = (
            (qa0, qa1), (ga0, ga1), (qb0, qb1), (st_out, st_in),
            (dq_out, dq_in), (ob_out, ob_in), (sb_out, sb_in),
        )[k]
        return remote(src, dst, mate_send.at[k], mate_recv.at[k], mate)

    kv_load(0, 0).wait()
    pl.semaphore_wait(barrier, count)
    give_all(0, 0)
    kv_load(0, 1).wait()
    give_all(0, 1)

    def rows_ready(i):
        for part in range(2):
            for h in range(heads):
                row_load(i, part, h).wait()
        to_mate(i).start()

    rows_ready(0)
    for j in range(2):
        kv_load(1, j).wait()
    for j in range(2):
        give_all(1, j)
    rows_ready(1)
    rows_ready(2)
    owner_load.wait()

    mine = (owner[me], owner[mate])

    def later(q, d):
        return (owner[2 * d + core] > mine[q]).astype(jnp.int32)

    lane = lax.broadcasted_iota(jnp.int32, (half, rows), 1) % half
    kept = lax.broadcasted_iota(jnp.int32, (half, rows), 0) <= lane

    def finish(e, m, tot, i, raw):
        top = jnp.max(raw, axis=0, keepdims=True)
        x = jnp.exp2(raw * factor - top * factor)
        e[i] = x
        m[i] = top
        tot[i] = jnp.sum(x, axis=0, keepdims=True)

    def pick(q, d, block):
        return jnp.where(later(q, d) == 1, block[half:], block[:half])

    def score_own(b, e, m, tot, queries):
        keys = kv[b, 0, chip]
        high = dot_nt(keys, queries[1])
        low = dot_nt(keys[:half], queries[0])
        finish(e, m, tot, 4 * chip, high[:half])
        finish(e, m, tot, 4 * chip + 1, jnp.where(kept, low, LOW))
        finish(e, m, tot, extra, jnp.where(kept, high[half:], LOW))

    def score(b, e, m, tot, q, d, queries):
        keys = kv[b, 0, d]
        finish(e, m, tot, 4 * d + 2 * q, dot_nt(keys[:half], queries[1]))
        finish(e, m, tot, 4 * d + 2 * q + 1, dot_nt(pick(q, d, keys), queries[later(q, d)]))

    def slope(i, x):
        pg[i] = x
        d_a[i] = jnp.sum(e_a[i] * x, axis=0, keepdims=True)

    def slope_own(grads):
        values = kv[0, 1, chip]
        high = dot_nt(values, grads[1])
        slope(4 * chip, high[:half])
        slope(4 * chip + 1, dot_nt(values[:half], grads[0]))
        slope(extra, high[half:])

    def slopes(q, d, grads):
        values = kv[0, 1, d]
        slope(4 * d + 2 * q, dot_nt(values[:half], grads[1]))
        slope(4 * d + 2 * q + 1, dot_nt(pick(q, d, values), grads[later(q, d)]))

    score_own(0, e_a, m_a, t_a, qa0)
    slope_own(ga0)
    to_mate(0).wait_recv()
    score(0, e_a, m_a, t_a, 1, chip, qa1)
    to_mate(1).wait_recv()
    slopes(1, chip, ga1)

    def keys_a(t):
        d = chip_at(t)
        take(0, 0, d)
        pass_on(0, 0, d)
        score(0, e_a, m_a, t_a, 0, d, qa0)
        score(0, e_a, m_a, t_a, 1, d, qa1)

    each(1, chips, keys_a)

    def values_a(t):
        d = chip_at(t)
        take(0, 1, d)
        pass_on(0, 1, d)
        slopes(0, d, ga0)
        slopes(1, d, ga1)

    each(1, chips, values_a)

    def combine(m, sums, out):
        for q in range(2):
            tops = [jnp.full((1, rows), LOW, F32) for _ in range(2)]
            for d in range(chips):
                i = 4 * d + 2 * q
                up = later(q, d) == 1
                tops[1] = jnp.maximum(tops[1], jnp.maximum(m[i], jnp.where(up, m[i + 1], LOW)))
                tops[0] = jnp.maximum(tops[0], jnp.where(up, LOW, m[i + 1]))
            if q == 0:
                tops[1] = jnp.maximum(tops[1], m[extra])
            acc = [[jnp.zeros((1, rows), F32) for _ in range(2)] for _ in sums]
            for d in range(chips):
                i = 4 * d + 2 * q
                up = later(q, d) == 1
                w1 = jnp.exp2((m[i] - tops[1]) * factor)
                w2 = jnp.exp2((m[i + 1] - jnp.where(up, tops[1], tops[0])) * factor)
                for a, s in zip(acc, sums):
                    second = s[i + 1] * w2
                    a[1] = a[1] + s[i] * w1 + jnp.where(up, second, 0.0)
                    a[0] = a[0] + jnp.where(up, 0.0, second)
            if q == 0:
                w1 = jnp.exp2((m[extra] - tops[1]) * factor)
                for a, s in zip(acc, sums):
                    a[1] = a[1] + s[extra] * w1
            for part in range(2):
                r = 2 * q + part
                out[r:r + 1] = tops[part]
                for k, a in enumerate(acc):
                    r = 4 * (k + 1) + 2 * q + part
                    out[r:r + 1] = a[part]

    combine(m_a, (t_a, d_a), st_out)
    to_mate(3).start()

    def relay_b(t):
        d = chip_at(t)

        @pl.when(is_near(d))
        def _():
            for j in range(2):
                take(1, j, d)
                forward(1, j, d).start()

    each(2, chips, relay_b)

    to_mate(3).wait_recv()
    for q in range(2):
        for part in range(2):
            r, s = 2 * q + part, 2 * (1 - q) + part
            m1, m2 = st_out[r:r + 1], st_in[s:s + 1]
            top = jnp.maximum(m1, m2)
            c1, c2 = jnp.exp2((m1 - top) * factor), jnp.exp2((m2 - top) * factor)
            inv = 1.0 / (st_out[4 + r:5 + r] * c1 + st_in[4 + s:5 + s] * c2)
            glob[r:r + 1] = top
            glob[4 + r:5 + r] = inv
            glob[8 + r:9 + r] = (st_out[8 + r:9 + r] * c1 + st_in[8 + s:9 + s] * c2) * inv

    def grad_item(i, stats):
        top, inv, delta = stats
        p = e_a[i] * (jnp.exp2((m_a[i] - top) * factor) * inv)
        return p.astype(BF16), (p * (pg[i] - delta)).astype(BF16)

    def stats_of(q, part):
        r = 2 * q + part
        return glob[r:r + 1], glob[4 + r:5 + r], glob[8 + r:9 + r]

    zero = jnp.zeros((half, rows), BF16)

    def grads(d, own):
        low, high = [0.0, 0.0], [0.0, 0.0]
        for q in range(2):
            side_rows = ((ga0, qa0), (ga1, qa1))[q]
            upper, lower = stats_of(q, 1), stats_of(q, 0)
            first = grad_item(4 * d + 2 * q, upper)
            sg_hi[q, d, 0:half] = first[1]
            if own and q == 0:
                second = grad_item(4 * d + 1, lower)
                third = grad_item(extra, upper)
                sg_hi[q, d, half:tok] = third[1]
                sg_lo[q, d] = second[1]
                for k in range(2):
                    low[k] += dot_nn(first[k], side_rows[k][1]) + dot_nn(second[k], side_rows[k][0])
                    high[k] += dot_nn(third[k], side_rows[k][1])
            else:
                at = later(q, d)
                up = at == 1
                second = grad_item(
                    4 * d + 2 * q + 1, [jnp.where(up, x, y) for x, y in zip(upper, lower)]
                )
                sg_hi[q, d, half:tok] = jnp.where(up, second[1], zero)
                sg_lo[q, d] = jnp.where(up, zero, second[1])
                for k in range(2):
                    r = dot_nn(second[k], side_rows[k][at])
                    low[k] += dot_nn(first[k], side_rows[k][1]) + jnp.where(up, 0.0, r)
                    high[k] += jnp.where(up, r, 0.0)
        return low, high

    def to_partner(k, d):
        return remote(
            gs.at[k, d], rp.at[k, d], p_send.at[k, d], p_recv.at[k, d], partner * 2 + core
        )

    def to_owner(k, d):
        return remote(
            ms.at[k, d], rf.at[k, pair], x_send.at[k, d], x_recv.at[k, pair], d * 2 + core
        )

    def merges(d):
        return jnp.logical_and(outside(d), is_near(d))

    def grads_away(u):
        d = chip_at(chips - 1 - u)
        low, high = grads(d, False)
        for k in range(2):
            gs[k, d, 0:half] = low[k].astype(BF16)
            gs[k, d, half:tok] = high[k].astype(BF16)
            gf[k, d, 0:half] = low[k]
            gf[k, d, half:tok] = high[k]

        @pl.when(jnp.logical_not(merges(d)))
        def _():
            for k in range(2):
                to_partner(k, d).start()

    each(0, chips - 1, grads_away)
    low, high = grads(chip, True)
    for k in range(2):
        gf[k, chip, 0:half] = low[k]
        gf[k, chip, half:tok] = high[k]

    def spread(hi, lo, left, q, out):
        out[1] = dot_tn(left.reshape(chips * tok, dim), hi[q].reshape(chips * tok, rows))
        out[0] = dot_tn(
            left[:, :half].reshape(chips * half, dim), lo[q].reshape(chips * half, rows)
        )

    keys_all = kv[0, 0]
    spread(sg_hi, sg_lo, keys_all, 1, dq_out)
    to_mate(4).start()
    spread(sg_hi, sg_lo, keys_all, 0, dq_own)

    score_own(1, e_b, m_b, t_b, qb0)
    to_mate(2).wait_recv()
    score(1, e_b, m_b, t_b, 1, chip, qb1)

    def keys_b(t):
        d = chip_at(t)

        @pl.when(jnp.logical_not(merges(d)))
        def _():
            for j in range(2):
                take(1, j, d)
        score(1, e_b, m_b, t_b, 0, d, qb0)
        score(1, e_b, m_b, t_b, 1, d, qb1)

    each(1, chips, keys_b)

    def merge(u):
        d = chip_at(chips - 1 - u)

        @pl.when(merges(d))
        def _():
            for k in range(2):
                to_partner(k, d).wait_recv()
                ms[k, d] = (gf[k, d] + rp[k, d].astype(F32)).astype(BF16)
                to_owner(k, d).start()

    each(0, chips - 2, merge)

    combine(m_b, (t_b,), sb_out)
    to_mate(6).start()

    def weigh(d):
        for q in range(2):
            i = 4 * d + 2 * q
            up = later(q, d) == 1
            lower, upper = (sb_out[2 * q + part:2 * q + part + 1] for part in range(2))
            w1 = jnp.exp2((m_b[i] - upper) * factor)
            w2 = jnp.exp2((m_b[i + 1] - jnp.where(up, upper, lower)) * factor)
            second = (e_b[i + 1] * w2).astype(BF16)
            p_hi[q, d, 0:half] = (e_b[i] * w1).astype(BF16)
            p_hi[q, d, half:tok] = jnp.where(up, second, zero)
            p_lo[q, d] = jnp.where(up, zero, second)

    each(0, chips, weigh)
    w = jnp.exp2((m_b[extra] - sb_out[1:2]) * factor)
    p_hi[0, chip, half:tok] = (e_b[extra] * w).astype(BF16)

    values_all = kv[1, 1]
    spread(p_hi, p_lo, values_all, 1, ob_out)
    to_mate(5).start()
    spread(p_hi, p_lo, values_all, 0, ob_own)

    def put(out, part, x):
        low = jnp.transpose(x).astype(BF16)
        for h in range(heads):
            out[part * half:(part + 1) * half, h * dim:(h + 1) * dim] = (
                low[h * half:(h + 1) * half]
            )

    to_mate(4).wait_recv()
    for part in range(2):
        put(out_dq, part, (dq_own[part] + dq_in[part]) * scale)

    to_mate(6).wait_recv()
    to_mate(5).wait_recv()
    for part in range(2):
        m1, m2 = sb_out[part:part + 1], sb_in[2 + part:3 + part]
        top = jnp.maximum(m1, m2)
        c1, c2 = jnp.exp2((m1 - top) * factor), jnp.exp2((m2 - top) * factor)
        inv = 1.0 / (sb_out[4 + part:5 + part] * c1 + sb_in[6 + part:7 + part] * c2)
        put(out_b, part, ob_own[part] * (c1 * inv) + ob_in[part] * (c2 * inv))

    for k in range(2):
        to_partner(k, chip).wait_recv()
        gf[k, chip] = gf[k, chip] + rp[k, chip].astype(F32)

    def add_far(u):
        other = lax.rem(pair + u, pairs)
        for k in range(2):
            remote(
                ms.at[k, chip], rf.at[k, other], x_send.at[k, chip], x_recv.at[k, other], mate
            ).wait_recv()
            gf[k, chip] = gf[k, chip] + rf[k, other].astype(F32)

    each(1, pairs, add_far)
    out_dv[...] = gf[0, chip].astype(BF16)
    out_dk[...] = (gf[1, chip] * scale).astype(BF16)

    for k in range(7):
        to_mate(k).wait_send()
    for b in range(2):
        for j in range(2):
            each(1, pairs, lambda k: give(b, j, nearest(k)).wait_send())
            give(b, j, partner).wait_send()

    def drain(t):
        d = chip_at(t)
        near = merges(d)

        @pl.when(near)
        def _():
            for b in range(2):
                for j in range(2):
                    forward(b, j, d).wait_send()
            for k in range(2):
                to_owner(k, d).wait_send()

        @pl.when(jnp.logical_not(near))
        def _():
            for k in range(2):
                to_partner(k, d).wait_send()

    each(1, chips, drain)


def emit(*refs):
    count = len(refs) // 2
    sems = refs[-1]
    copies = [
        pltpu.make_async_copy(refs[i], refs[count + i], sems.at[i]) for i in range(count)
    ]
    for copy in copies:
        copy.start()
    for copy in copies:
        copy.wait()


def on_device(n, qa, ka, va, ga, qb, kb, vb, owner):
    tok, dim = ka.shape
    heads = qa.shape[1] // dim
    chips = n // 2
    pairs = chips // 2
    half = tok // 2
    rows = heads * half
    items = 4 * chips + 1
    any_spec = pl.BlockSpec(memory_space=pl.ANY)
    vmem_spec = pl.BlockSpec(memory_space=pltpu.VMEM)
    dma = pltpu.SemaphoreType.DMA
    vmem = pltpu.VMEM
    queries = vmem((2, rows, dim), BF16)
    block = vmem((items, half, rows), F32)
    line = vmem((items, 1, rows), F32)
    stats = vmem((16, rows), F32)
    high = vmem((2, chips, tok, rows), BF16)
    low = vmem((2, chips, half, rows), BF16)
    turned = vmem((2, dim, rows), F32)
    outs = pl.pallas_call(
        functools.partial(kernel, n, tok, heads, dim),
        out_shape=(
            pltpu.VMEM(qb.shape, BF16),
            pltpu.VMEM(qa.shape, BF16),
            pltpu.VMEM(ka.shape, BF16),
            pltpu.VMEM(va.shape, BF16),
        ),
        in_specs=[any_spec] * 8,
        out_specs=(vmem_spec,) * 4,
        scratch_shapes=[
            pltpu.SMEM(owner.shape, jnp.int32),
            vmem((2, 2, chips, tok, dim), BF16),
            queries, queries, queries, queries, queries, queries,
            block, block, block,
            line, line, line, line, line,
            stats, stats, stats, stats, stats,
            high, low, high, low,
            turned, turned, turned, turned, turned, turned,
            vmem((2, chips, tok, dim), F32),
            vmem((2, chips, tok, dim), BF16),
            vmem((2, chips, tok, dim), BF16),
            vmem((2, chips, tok, dim), BF16),
            vmem((2, pairs, tok, dim), BF16),
            dma((5 + 6 * heads,)),
            dma((2, 2, chips)),
            dma((2, 2, chips)),
            dma((2, 2, chips)),
            dma((7,)),
            dma((7,)),
            dma((2, chips)),
            dma((2, chips)),
            dma((2, chips)),
            dma((2, pairs)),
        ],
        compiler_params=pltpu.CompilerParams(collective_id=0, has_side_effects=True),
    )(owner, qa, ka, va, ga, qb, kb, vb)
    return pl.pallas_call(
        emit,
        out_shape=tuple(jax.ShapeDtypeStruct(x.shape, x.dtype) for x in outs),
        in_specs=[vmem_spec] * 4,
        out_specs=(any_spec,) * 4,
        scratch_shapes=[dma((4,))],
        compiler_params=pltpu.CompilerParams(vmem_limit_bytes=8 * 2**20),
    )(*outs)


def solution(mesh):
    spec = P(("dp", "context"), "tensor")
    return jax.shard_map(
        functools.partial(on_device, mesh.shape["context"]),
        mesh=mesh,
        in_specs=(spec,) * 7 + (P(),),
        out_specs=(spec,) * 4,
        check_vma=False,
    )
```
